32 devices in a mesh: cluster: 8 (over z, y), client: 4 (over x, core).
Axes of the slice: x: 2, y: 2, z: 4, core: 2. Of those that a mesh axis runs over, the one named last changes fastest.
Arguments:
- user_feats: bfloat16 [6144, 2048], P('client'), may hold values from -6 to 6
- item_feats: bfloat16 [6144, 2048], P('client'), may hold values from -6 to 6
- item_ids: int32 [6144], P('client'), may hold values from 0 to 999
- picks: int32 [64], P('client'), may hold values from 0 to 7
- user_weight: bfloat16 [8, 2048, 512], P('cluster'), may hold values from -0.125 to 0.125
- item_weight: bfloat16 [8, 2048, 512], P('cluster'), may hold values from -0.125 to 0.125
Outputs:
- loss_table: float32 [64, 8], P('client')
- user_grad: float32 [8, 2048, 512], P('cluster', 'client')
- item_grad: float32 [8, 2048, 512], P('cluster', 'client')
The draws below stay inside these ranges and needn't reach their ends.
Inputs may be any that keep to these rules, and one draw needn't show every extreme that they name: `picks`: one cluster per client.
All inputs are finite; a program needn't handle non-finite values.
Results may differ from the reference program's by a relative error of at most 0.005.
Values sent between devices are 32-bit elements; how exact they have to be, the bound alone decides.
No kernel may reach another device: no remote copies, remote signals or barrier semaphores. Data moves between devices by JAX's collectives and lax.ppermute only.
A program may use at most 128 MiB of HBM per device.

```python
import math
import jax
import jax.numpy as jnp
import numpy as np
from jax import lax

D = 2048
E = 512
R = 96
CLIENTS = 64
CLUSTERS = 8


def with_ends(entries, stream_key, least, top_value):
    longest = entries.shape.index(max(entries.shape))
    spots = []
    for shift in (0, 1):
        where = [jax.random.randint(jax.random.fold_in(stream_key, axis), (), 0, length) for axis, length in enumerate(entries.shape)]
        where[longest] = (where[longest] + shift) % entries.shape[longest]
        spots.append(tuple(where))
    return entries.at[spots[0]].set(least).at[spots[1]].set(top_value)


def raised(result, own_key, source, target, shards_of, factor):
    owner, partner = [(jnp.arange(result.shape[axis_at]) // (result.shape[axis_at] // shards_of)).reshape([-1 if axis == axis_at else 1 for axis in range(result.ndim)]) for axis_at in (source, target)]
    chosen = jax.random.permutation(own_key, shards_of)[partner]
    strong = (owner == chosen) | (owner == (partner + shards_of // 2) % shards_of)
    return jnp.where(strong, factor * result, result)


def block_scale(own_key, dims, shards, least, largest):
    def one(dim, parts):
        draws = jax.random.uniform(jax.random.fold_in(jax.random.fold_in(own_key, 6), dim), (parts,), jnp.float32, least / len(shards), largest / len(shards))
        return jnp.repeat(jnp.exp(draws), dims[dim] // parts).reshape((-1,) + (1,) * (len(dims) - dim - 1))

    factor_of = one(*shards[0])
    for cut in shards[1:]:
        factor_of = factor_of * one(*cut)
    return factor_of


def rank_bounds(count, lean):
    weights = [(1 << 20) // math.isqrt(standing ** lean) + 1 for standing in range(1, count + 1)]
    spread = 1 + sum(weights) // (1 << 30)
    return np.cumsum(np.array([max(1, weight // spread) for weight in weights]))


def ranked_ids(rng, extent, number_of, skew):
    listing = rank_bounds(number_of, skew)
    lot = jax.random.randint(jax.random.fold_in(rng, 1), extent, 0, int(listing[number_of - 1]))
    standing = jnp.searchsorted(jnp.asarray(listing, jnp.int32), lot, side="right")
    return jax.random.permutation(jax.random.fold_in(rng, 2), number_of)[standing].astype(jnp.int32)


def gaussian(own_key, shape, spread, reach, split=(), held_as=jnp.bfloat16):
    drawn = spread * jax.random.normal(own_key, shape, jnp.float32)
    if split:
        drawn = drawn * block_scale(own_key, shape, split, -0.22, 0.18)
    return jnp.clip(drawn, -reach, reach).astype(held_as)


def gaussian_with(stream_key, extent, width, reach, cuts, heavy, kind=jnp.bfloat16):
    array = width * jax.random.normal(stream_key, extent, jnp.float32)
    if cuts:
        array = array * block_scale(stream_key, extent, cuts, -0.22, 0.18)
    return jnp.clip(raised(array, jax.random.fold_in(stream_key, 3), *heavy), -reach, reach).astype(kind)


def setup_inputs(seed: int = 0) -> dict:
    arg_keys = jax.random.split(jax.random.key(seed), 7)
    user_feats = gaussian_with(arg_keys[0], (CLIENTS * R, D), 1.0, 6.0, ((0, 4),), (0, 1, 4, 2.0))
    item_feats = gaussian_with(arg_keys[1], (CLIENTS * R, D), 1.0, 6.0, ((0, 4),), (0, 1, 4, 2.0))
    item_ids = with_ends(ranked_ids(arg_keys[2], (CLIENTS * R,), 1000, 2), jax.random.fold_in(arg_keys[2], 3), 0, 999).astype(jnp.int32)
    picks = with_ends(ranked_ids(arg_keys[3], (CLIENTS,), CLUSTERS, 1), jax.random.fold_in(arg_keys[3], 3), 0, CLUSTERS - 1).astype(jnp.int32)
    user_weight = gaussian(arg_keys[4], (CLUSTERS, D, E), D ** -0.5, 0.125, ((0, 8),))
    item_weight = gaussian(arg_keys[5], (CLUSTERS, D, E), D ** -0.5, 0.125, ((0, 8),))
    return dict(user_feats=user_feats, item_feats=item_feats, item_ids=item_ids, picks=picks, user_weight=user_weight, item_weight=item_weight)


def silu_slope(pre_act):
    sig = jax.nn.sigmoid(pre_act)
    return sig * (1.0 + pre_act * (1.0 - sig))

def contract_rows(left, right):
    return lax.dot_general(left, right, (((0,), (0,)), ((), ())), preferred_element_type=jnp.float32)

def reference(user_feats, item_feats, item_ids, picks, user_weight, item_weight):
    temper = 1.0 / math.sqrt(E)
    grouped = item_ids.reshape(CLIENTS, R)
    labels = (grouped[:, :, None] == grouped[:, None, :]).astype(jnp.float32)

    def per_cluster(cluster_index):
        user_map = user_weight[cluster_index]
        item_map = item_weight[cluster_index]
        pre_user = jnp.dot(user_feats, user_map, preferred_element_type=jnp.float32)
        user_vec = jax.nn.silu(pre_user).astype(jnp.bfloat16)
        item_vec = jnp.dot(item_feats, item_map, preferred_element_type=jnp.float32).astype(jnp.bfloat16)
        user_blocks = lax.optimization_barrier(user_vec).astype(jnp.float32).reshape(CLIENTS, R, E)
        item_blocks = lax.optimization_barrier(item_vec).astype(jnp.float32).reshape(CLIENTS, R, E)
        scores = jnp.einsum('cre,cte->crt', user_blocks, item_blocks) * temper
        pair_loss = jax.nn.softplus(scores) - labels * scores
        client_loss = lax.optimization_barrier(jnp.mean(pair_loss, axis=(1, 2)))
        chosen = (picks == cluster_index).astype(jnp.float32)
        slope = ((jax.nn.sigmoid(scores) - labels) * temper * chosen[:, None, None]).astype(jnp.bfloat16)
        slope = lax.optimization_barrier(slope).astype(jnp.float32)
        user_slope = jnp.einsum('crt,cte->cre', slope, item_blocks).reshape(CLIENTS * R, E)
        pre_slope = (user_slope * silu_slope(pre_user)).astype(jnp.bfloat16)
        item_slope = jnp.einsum('crt,cre->cte', slope, user_blocks).reshape(CLIENTS * R, E).astype(jnp.bfloat16)
        grad_user = contract_rows(user_feats, pre_slope)
        grad_item = contract_rows(item_feats, item_slope)
        return (client_loss, grad_user, grad_item)
    losses, grad_user, grad_item = lax.map(per_cluster, jnp.arange(CLUSTERS, dtype=jnp.int32))
    return (losses.T, grad_user, grad_item)
```

```python
import functools
import math

import jax
import jax.numpy as jnp
from jax import lax
from jax.experimental import pallas as pl
from jax.experimental.pallas import tpu as pltpu
from jax.sharding import PartitionSpec as P

GROUP = 4
LANES = 128
VMEM_BYTES = 40 * 1024 * 1024


def contract_rows(left, right):
    return lax.dot_general(
        left, right, (((0,), (0,)), ((), ())), preferred_element_type=jnp.float32
    )


def contract_lanes(left, right):
    return lax.dot_general(
        left, right, (((1,), (1,)), ((), ())), preferred_element_type=jnp.float32
    )


def dot(left, right):
    return jnp.dot(left, right, preferred_element_type=jnp.float32)


def order_clients(picks_s, slots_s, clients, mine):
    chosen = jnp.int32(0)
    for c in range(clients):
        slots_s[chosen] = jnp.int32(c)
        chosen = chosen + (picks_s[c] == mine).astype(jnp.int32)
    last = chosen
    for c in range(clients):
        slots_s[last] = jnp.int32(c)
        last = last + (picks_s[c] != mine).astype(jnp.int32)
    return chosen


def label_block(ids_v, client, per):
    start = client * per
    row_at, off = start // LANES, start % LANES
    next_at = jnp.minimum(row_at + 1, ids_v.shape[0] - 1)
    lane = lax.broadcasted_iota(jnp.int32, (1, LANES), 1)
    turn = (LANES - off) % LANES
    here = pltpu.roll(ids_v[pl.ds(row_at, 1), :], turn, 1)
    there = pltpu.roll(ids_v[pl.ds(next_at, 1), :], turn, 1)
    row = jnp.where(lane < LANES - off, here, there).astype(jnp.float32)
    wide = jnp.broadcast_to(row, (per, LANES))
    diagonal = lax.broadcasted_iota(jnp.int32, (per, LANES), 0) == lax.broadcasted_iota(
        jnp.int32, (per, LANES), 1
    )
    column = jnp.sum(jnp.where(diagonal, wide, 0.0), axis=1, keepdims=True)
    return jnp.where(wide[:, :per] == column, 1.0, 0.0)


def forward_block(block, base, waits, feats, weights, scratch, slots_s, ids_v, loss_v, mine, per, chosen, slopes):
    user_rows, item_rows = feats
    pre_v, user_v, item_v = scratch
    rows = pre_v.shape[0]
    group = rows // per
    width = pre_v.shape[1]
    temper = 1.0 / math.sqrt(width)
    pieces = len(waits)
    depth = user_rows.shape[1] // pieces
    totals = []
    for tower in range(2):
        total = None
        for piece in range(pieces):
            waits[piece](tower)
            cols = slice(piece * depth, (piece + 1) * depth)
            part = dot(feats[tower][pl.ds(base, rows), cols], weights[tower][cols, :])
            total = part if total is None else total + part
        totals.append(total)
        if tower == 0:
            pre_v[...] = total
            user_v[...] = (total * jax.nn.sigmoid(total)).astype(jnp.bfloat16)
        else:
            item_v[...] = total.astype(jnp.bfloat16)
    lane = lax.broadcasted_iota(jnp.int32, (1, LANES), 1)
    for i in range(group):
        slot = block * group + i
        client = slots_s[slot]
        own = slice(i * per, (i + 1) * per)
        user, item = user_v[own, :], item_v[own, :]
        scores = contract_lanes(user, item) * temper
        labels = label_block(ids_v, client, per)
        soft = jnp.maximum(scores, 0.0) + jnp.log1p(jnp.exp(-jnp.abs(scores)))
        pair = soft - labels * scores
        loss = jnp.sum(jnp.sum(pair, axis=1, keepdims=True), axis=0, keepdims=True) / (per * per)
        loss_v[pl.ds(client, 1), :] = jnp.where(lane == mine, jnp.broadcast_to(loss, (1, LANES)), 0.0)
        if slopes is not None:
            user_slopes, item_slopes = slopes
            live = jnp.where(slot < chosen, temper, 0.0)
            slope = ((jax.nn.sigmoid(scores) - labels) * live).astype(jnp.bfloat16)
            pre = pre_v[own, :]
            sig = jax.nn.sigmoid(pre)
            at = pl.ds(base + i * per, per)
            user_slopes[at, :] = (dot(slope, item) * (sig * (1.0 + pre * (1.0 - sig)))).astype(jnp.bfloat16)
            item_slopes[at, :] = contract_rows(slope, user).astype(jnp.bfloat16)


def fetch_weights(user_weight, item_weight, weights, sems, pieces):
    def copy(tower, piece):
        depth = weights[tower].shape[0] // pieces
        cut = pl.ds(piece * depth, depth)
        source = (user_weight, item_weight)[tower]
        return pltpu.make_async_copy(source.at[0, cut, :], weights[tower].at[cut, :], sems.at[tower, piece])

    return copy


def fetch_feats(client, base, user_feats, item_feats, feats, per, pieces):
    def copy(tower, piece, sem):
        depth = feats[tower].shape[1] // pieces
        cut = slice(piece * depth, (piece + 1) * depth)
        source = (user_feats, item_feats)[tower]
        return pltpu.make_async_copy(
            source.at[pl.ds(client * per, per), cut], feats[tower].at[pl.ds(base, per), cut], sem
        )

    return copy


def sum_terms(feats, slopes, blocks, span, cols, groups, rows, out, at):
    wide = cols.stop - cols.start
    for j, block in enumerate(blocks):
        place = (slice(j * span, (j + 1) * span), slice(at, at + wide))
        part_of = pl.ds(pl.multiple_of(block * span, span), span)
        out[place] = contract_rows(feats[0:rows, part_of], slopes[0:rows, cols])

        def more(g, carry):
            these = pl.ds(pl.multiple_of(g * rows, rows), rows)
            out[place] += contract_rows(feats[these, part_of], slopes[these, cols])
            return carry

        lax.fori_loop(1, groups, more, 0)


def relative_blocks(shards, flip):
    me = lax.axis_index("client")
    return [jnp.bitwise_xor(me, (j << 1) ^ flip) for j in range(shards // 4)]


def first_kernel(
    sizes, picks, ids_h, user_feats, item_feats, user_weight, item_weight,
    user_rows, item_rows, user_slopes, item_slopes, loss_v, count_v, give, keep,
    picks_s, slots_s, ids_v, user_w, item_w, pre_v, user_v, item_v, small_sem, weight_sem, feat_sem,
):
    clients, per, group, pieces, shards, head = sizes
    rows = group * per
    mine = lax.axis_index("cluster")
    weights, feats = (user_w, item_w), (user_rows, item_rows)
    get_picks = pltpu.make_async_copy(picks, picks_s, small_sem.at[0])
    get_ids = pltpu.make_async_copy(ids_h, ids_v, small_sem.at[1])
    get_picks.start()
    weight_copy = fetch_weights(user_weight, item_weight, weights, weight_sem, pieces)
    for tower in range(2):
        for piece in range(pieces):
            weight_copy(tower, piece).start()
    get_picks.wait()
    chosen = order_clients(picks_s, slots_s, clients, mine)
    groups = jnp.maximum(1, (chosen + group - 1) // group)

    def start_group(g, carry):
        for tower in range(2):
            for piece in range(pieces):
                for i in range(group):
                    slot = g * group + i
                    copy = fetch_feats(slots_s[slot], slot * per, user_feats, item_feats, feats, per, pieces)
                    copy(tower, piece, feat_sem.at[g, tower, piece]).start()
        return carry

    start_group(0, 0)
    get_ids.start()
    lax.fori_loop(1, groups, start_group, 0)
    count_v[...] = jnp.broadcast_to(groups.astype(jnp.float32), count_v.shape)
    get_ids.wait()

    def run_group(g, first):
        base = g * rows if first else pl.multiple_of(g * rows, rows)

        def wait_for(piece):
            def wait(tower):
                if first:
                    weight_copy(tower, piece).wait()
                depth = feats[tower].shape[1] // pieces
                whole = feats[tower].at[pl.ds(base, rows), piece * depth : (piece + 1) * depth]
                pltpu.make_async_copy(whole, whole, feat_sem.at[g, tower, piece]).wait()

            return wait

        forward_block(
            g, base, [wait_for(piece) for piece in range(pieces)], feats, weights,
            (pre_v, user_v, item_v), slots_s, ids_v, loss_v, mine, per, chosen, (user_slopes, item_slopes),
        )

    run_group(0, True)

    def more_groups(g, carry):
        run_group(g, False)
        return carry

    lax.fori_loop(1, groups, more_groups, 0)
    top = shards // 2
    span = user_rows.shape[1] // shards
    for out, flip in ((give, top ^ 1), (keep, top)):
        sum_terms(user_rows, user_slopes, relative_blocks(shards, flip), span, slice(0, head), groups, rows, out, 0)


def terms_kernel(sizes, user_rows, item_rows, user_slopes, item_slopes, count_v, after, give, *keeps):
    rows, shards, flip, skip = sizes
    del after
    groups = jnp.max(count_v[...]).astype(jnp.int32)
    span = user_rows.shape[1] // shards
    width = user_slopes.shape[1]
    towers = ((user_rows, user_slopes, slice(skip, width)), (item_rows, item_slopes, slice(0, width)))
    at = 0
    for tower, (feats, slopes, cols) in enumerate(towers):
        sum_terms(feats, slopes, relative_blocks(shards, flip ^ 1), span, cols, groups, rows, give, at)
        sum_terms(feats, slopes, relative_blocks(shards, flip), span, cols, groups, rows, keeps[tower], 0)
        at += cols.stop - cols.start


def loss_kernel(
    sizes, picks, ids_v, user_feats, item_feats, user_weight, item_weight, count_v, loss_in, after,
    loss_v, picks_s, slots_s, user_rows, item_rows, user_w, item_w, pre_v, user_v, item_v, weight_sem, feat_sem,
):
    clients, per, group = sizes
    del after
    rows = group * per
    mine = lax.axis_index("cluster")
    weights, feats = (user_w, item_w), (user_rows, item_rows)
    weight_copy = fetch_weights(user_weight, item_weight, weights, weight_sem, 1)
    weight_copy(0, 0).start()
    weight_copy(1, 0).start()
    loss_v[...] = loss_in[...]
    for c in range(clients):
        picks_s[c] = picks[c]
    chosen = order_clients(picks_s, slots_s, clients, mine)
    groups = jnp.max(count_v[...]).astype(jnp.int32)
    weight_copy(0, 0).wait()
    weight_copy(1, 0).wait()

    def run_group(g, carry):
        for i in range(group):
            copy = fetch_feats(slots_s[g * group + i], i * per, user_feats, item_feats, feats, per, 1)
            for tower in range(2):
                copy(tower, 0, feat_sem.at[tower]).start()

        def wait(tower):
            pltpu.make_async_copy(feats[tower], feats[tower], feat_sem.at[tower]).wait()

        forward_block(
            g, 0, [wait], feats, weights, (pre_v, user_v, item_v), slots_s, ids_v, loss_v, mine, per, chosen, None
        )
        return carry

    lax.fori_loop(groups, clients // group, run_group, 0)


def swapped(value, axis, mask, size):
    return lax.ppermute(value, axis, [(i, i ^ mask) for i in range(size)])


def in_vmem(value):
    return pltpu.with_memory_space_constraint(value, pltpu.VMEM)


def body(sizes, user_feats, item_feats, item_ids, picks, user_weight, item_weight):
    shards, clusters = sizes
    clients = picks.shape[0]
    row_count, depth = user_feats.shape
    per = row_count // clients
    width = user_weight.shape[2]
    group = math.gcd(clients, GROUP)
    rows = group * per
    pieces = 2
    head = width // 2
    top = shards // 2
    quarter = depth // 4
    assert shards & (shards - 1) == 0 and shards >= 4 and per <= LANES and clusters <= LANES

    ids = item_ids.reshape(-1, LANES)
    bf16, f32, i32 = jnp.bfloat16, jnp.float32, jnp.int32
    anywhere = pl.BlockSpec(memory_space=pl.ANY)
    vmem = pl.BlockSpec(memory_space=pltpu.VMEM)
    smem = pl.BlockSpec(memory_space=pltpu.SMEM)
    params = pltpu.CompilerParams(vmem_limit_bytes=VMEM_BYTES)
    flops = 2 * rows * depth * width

    def cost(factor):
        return pl.CostEstimate(flops=int(factor * flops), bytes_accessed=1 << 20, transcendentals=0)

    towers = [
        pltpu.VMEM((depth, width), bf16),
        pltpu.VMEM((depth, width), bf16),
        pltpu.VMEM((rows, width), f32),
        pltpu.VMEM((rows, width), bf16),
        pltpu.VMEM((rows, width), bf16),
    ]
    user_rows, item_rows, user_slopes, item_slopes, loss, count, give, keep = pl.pallas_call(
        functools.partial(first_kernel, (clients, per, group, pieces, shards, head)),
        out_shape=[
            pltpu.VMEM((row_count, depth), bf16),
            pltpu.VMEM((row_count, depth), bf16),
            pltpu.VMEM((row_count, width), bf16),
            pltpu.VMEM((row_count, width), bf16),
            pltpu.VMEM((clients, LANES), f32),
            pltpu.VMEM((8, LANES), f32),
            pltpu.VMEM((quarter, head), f32),
            pltpu.VMEM((quarter, head), f32),
        ],
        in_specs=[anywhere] * 6,
        out_specs=[vmem] * 8,
        scratch_shapes=[
            pltpu.SMEM((clients,), i32),
            pltpu.SMEM((clients + 1,), i32),
            pltpu.VMEM(ids.shape, i32),
            *towers,
            pltpu.SemaphoreType.DMA((2,)),
            pltpu.SemaphoreType.DMA((2, pieces)),
            pltpu.SemaphoreType.DMA((clients // group, 2, pieces)),
        ],
        compiler_params=params,
        cost_estimate=cost(6),
        name="first",
    )(picks, ids, user_feats, item_feats, user_weight, item_weight)

    def terms(flip, skip, after, name):
        return pl.pallas_call(
            functools.partial(terms_kernel, (rows, shards, flip, skip)),
            out_shape=[
                pltpu.VMEM((quarter, 2 * width - skip), f32),
                pltpu.VMEM((quarter, width - skip), f32),
                pltpu.VMEM((quarter, width), f32),
            ],
            in_specs=[vmem] * 5 + [anywhere],
            out_specs=[vmem] * 3,
            compiler_params=params,
            cost_estimate=cost(2),
            name=name,
        )(in_vmem(user_rows), in_vmem(item_rows), in_vmem(user_slopes), in_vmem(item_slopes), in_vmem(count), after)

    first_sum = swapped(give, "client", 1, shards) + keep
    from_first = swapped(first_sum, "client", top, shards)

    give, keep_user, keep_item = terms(top, head, count, "away_terms")
    got = swapped(give, "client", 1, shards)
    second_sum = got[:, : width - head] + keep_user
    third_sum = got[:, width - head :] + keep_item
    from_second = swapped(second_sum, "client", top, shards)
    from_third = swapped(third_sum, "client", top, shards)

    give, keep_user, keep_item = terms(0, 0, first_sum, "home_terms")
    got = swapped(give, "client", 1, shards)
    home_user = got[:, :width] + keep_user
    home_item = got[:, width:] + keep_item

    loss = pl.pallas_call(
        functools.partial(loss_kernel, (clients, per, group)),
        out_shape=jax.ShapeDtypeStruct((clients, LANES), f32),
        in_specs=[smem, vmem] + [anywhere] * 4 + [vmem, vmem, anywhere],
        out_specs=vmem,
        scratch_shapes=[
            pltpu.SMEM((clients,), i32),
            pltpu.SMEM((clients + 1,), i32),
            pltpu.VMEM((rows, depth), bf16),
            pltpu.VMEM((rows, depth), bf16),
            *towers,
            pltpu.SemaphoreType.DMA((2, 1)),
            pltpu.SemaphoreType.DMA((2,)),
        ],
        compiler_params=params,
        cost_estimate=cost(6),
        name="loss",
    )(picks, ids, user_feats, item_feats, user_weight, item_weight, in_vmem(count), in_vmem(loss), third_sum)
    mask = 1
    while mask < clusters:
        loss = loss + swapped(loss, "cluster", mask, clusters)
        mask *= 2
    loss_table = loss[:, :clusters]

    user_grad = home_user + jnp.concatenate([from_first, from_second], axis=1)
    item_grad = home_item + from_third
    half = shards // 4
    while half > 1:
        half //= 2
        cut = half * (depth // shards)
        mask = half << 1
        user_grad = user_grad[:cut] + swapped(user_grad[cut:], "client", mask, shards)
        item_grad = item_grad[:cut] + swapped(item_grad[cut:], "client", mask, shards)
    return loss_table, user_grad[None], item_grad[None]


def solution(mesh):
    in_specs = (
        P("client", None),
        P("client", None),
        P("client"),
        P("client"),
        P("cluster", None, None),
        P("cluster", None, None),
    )
    out_specs = (P("client", None), P("cluster", "client", None), P("cluster", "client", None))
    sizes = (mesh.shape["client"], mesh.shape["cluster"])
    return jax.shard_map(
        functools.partial(body, sizes), mesh=mesh, in_specs=in_specs, out_specs=out_specs, check_vma=False
    )
```

```python
import functools
import math

import jax
import jax.numpy as jnp
from jax import lax
from jax.experimental import pallas as pl
from jax.experimental.pallas import tpu as pltpu
from jax.sharding import PartitionSpec as P


GROUP = 4
EXACT = 8
LANES = 128


def contract_rows(left, right):
    return lax.dot_general(
        left, right, (((0,), (0,)), ((), ())), preferred_element_type=jnp.float32
    )


def contract_lanes(left, right):
    return lax.dot_general(
        left, right, (((1,), (1,)), ((), ())), preferred_element_type=jnp.float32
    )


def dot(left, right):
    return jnp.dot(left, right, preferred_element_type=jnp.float32)


def order_clients(picks_s, slots_s, clients, mine):
    chosen = jnp.int32(0)
    for c in range(clients):
        slots_s[chosen] = jnp.int32(c)
        chosen = chosen + (picks_s[c] == mine).astype(jnp.int32)
    last = chosen
    for c in range(clients):
        slots_s[last] = jnp.int32(c)
        last = last + (picks_s[c] != mine).astype(jnp.int32)
    return chosen


def label_block(ids_v, client, per):
    start = client * per
    row_at, off = start // LANES, start % LANES
    next_at = jnp.minimum(row_at + 1, ids_v.shape[0] - 1)
    lane = lax.broadcasted_iota(jnp.int32, (1, LANES), 1)
    turn = (LANES - off) % LANES
    here = pltpu.roll(ids_v[pl.ds(row_at, 1), :], turn, 1)
    there = pltpu.roll(ids_v[pl.ds(next_at, 1), :], turn, 1)
    row = jnp.where(lane < LANES - off, here, there).astype(jnp.float32)
    wide = jnp.broadcast_to(row, (per, LANES))
    diagonal = lax.broadcasted_iota(jnp.int32, (per, LANES), 0) == lax.broadcasted_iota(
        jnp.int32, (per, LANES), 1
    )
    column = jnp.sum(jnp.where(diagonal, wide, 0.0), axis=1, keepdims=True)
    return jnp.where(wide[:, :per] == column, 1.0, 0.0)


def run_user(at, feats, weight, user_v, bend_v):
    pre = dot(feats[at, :], weight[...])
    sig = jax.nn.sigmoid(pre)
    user_v[at, :] = (pre * sig).astype(jnp.bfloat16)
    if bend_v is not None:
        bend_v[at, :] = sig * (1.0 + pre * (1.0 - sig))


def run_item(at, feats, weight, item_v):
    item_v[at, :] = dot(feats[at, :], weight[...]).astype(jnp.bfloat16)


def scores_of(vectors, starts, per, temper):
    user_v, item_v = vectors
    users = [user_v[pl.ds(start, per), :] for start in starts]
    items = [item_v[pl.ds(start, per), :] for start in starts]
    scores = [contract_lanes(user, item) * temper for user, item in zip(users, items)]
    return users, items, scores


def run_slopes(base, slot, group, per, chosen, vectors, bend_v, label_v, slopes):
    user_slopes, item_slopes = slopes
    temper = 1.0 / math.sqrt(bend_v.shape[1])
    starts = [base + i * per for i in range(group)]
    users, items, scores = scores_of(vectors, starts, per, temper)
    slope = [
        ((jax.nn.sigmoid(score) - label_v[pl.ds(start, per), :per]) * jnp.where(slot + i < chosen, temper, 0.0)).astype(
            jnp.bfloat16
        )
        for i, (score, start) in enumerate(zip(scores, starts))
    ]
    for i, start in enumerate(starts):
        user_slopes[pl.ds(start, per), :] = (dot(slope[i], items[i]) * bend_v[pl.ds(start, per), :]).astype(jnp.bfloat16)
    for i, start in enumerate(starts):
        item_slopes[pl.ds(start, per), :] = contract_rows(slope[i], users[i]).astype(jnp.bfloat16)


def add_terms(feats, slopes, targets, span, cols, these, at, fresh):
    wide = cols.stop - cols.start
    for blocks, out in targets:
        for j, block in enumerate(blocks):
            place = (slice(j * span, (j + 1) * span), slice(at, at + wide))
            part_of = pl.ds(pl.multiple_of(block * span, span), span)
            part = contract_rows(feats[these, part_of], slopes[these, cols])
            out[place] = part if fresh else out[place] + part


def sum_terms(feats, slopes, targets, span, cols, groups, rows, at):
    @pl.when(groups == 1)
    def _():
        add_terms(feats, slopes, targets, span, cols, slice(0, rows), at, True)

    @pl.when(groups > 1)
    def _():
        add_terms(feats, slopes, targets, span, cols, slice(0, 2 * rows), at, True)

        def more(g, carry):
            add_terms(feats, slopes, targets, span, cols, pl.ds(pl.multiple_of(g * rows, rows), rows), at, False)
            return carry

        lax.fori_loop(2, groups, more, 0)


def relative_blocks(shards, flip):
    me = lax.axis_index("client")
    return [jnp.bitwise_xor(me, (j << 1) ^ flip) for j in range(shards // 4)]


def first_kernel(
    sizes, picks, ids_h, user_feats, item_feats, user_weight, item_weight,
    user_rows, item_rows, user_slopes, item_slopes, count_v, give, keep,
    picks_s, slots_s, ids_v, label_v, user_w, item_w, bend_v, user_v, item_v, small_sem, weight_sem, feat_sem,
):
    clients, per, group, shards, head = sizes
    rows = group * per
    mine = lax.axis_index("cluster")
    get_picks = pltpu.make_async_copy(picks, picks_s, small_sem.at[0])
    get_ids = pltpu.make_async_copy(ids_h, ids_v, small_sem.at[1])
    get_user_w = pltpu.make_async_copy(user_weight.at[0], user_w, weight_sem.at[0])
    get_item_w = pltpu.make_async_copy(item_weight.at[0], item_w, weight_sem.at[1])
    get_picks.start()
    get_user_w.start()
    get_picks.wait()
    chosen = order_clients(picks_s, slots_s, clients, mine)
    live = jnp.maximum(1, chosen)
    groups = (live + group - 1) // group
    feats, slopes = (user_rows, item_rows), (user_slopes, item_slopes)

    def place_of(slot):
        return pl.ds(pl.multiple_of(slot * per, per), per)

    def get_rows(tower, slot):
        source = (user_feats, item_feats)[tower]
        return pltpu.make_async_copy(
            source.at[place_of(slots_s[slot]), :], feats[tower].at[place_of(slot), :], feat_sem.at[tower, slot]
        )

    def start_rows(tower):
        def start(slot, carry):
            get_rows(tower, slot).start()
            return carry

        lax.fori_loop(0, live, start, 0)

    start_rows(0)
    get_item_w.start()
    start_rows(1)
    get_ids.start()
    count_v[...] = jnp.broadcast_to(groups.astype(jnp.float32), count_v.shape)

    def clear(slot, carry):
        for tower in range(2):
            feats[tower][place_of(slot), :] = jnp.zeros((per, user_rows.shape[1]), jnp.bfloat16)
            slopes[tower][place_of(slot), :] = jnp.zeros((per, user_slopes.shape[1]), jnp.bfloat16)
        return carry

    lax.fori_loop(live, groups * group, clear, 0)
    get_ids.wait()

    def label_group(g, carry):
        for i in range(group):
            slot = g * group + i
            label_v[place_of(slot), :per] = label_block(ids_v, slots_s[slot], per)
        return carry

    lax.fori_loop(0, groups, label_group, 0)

    top = shards // 2
    span = user_rows.shape[1] // shards
    targets = ((relative_blocks(shards, top ^ 1), give), (relative_blocks(shards, top), keep))

    def slopes_of(base, slot, number):
        run_slopes(base, slot, number, per, chosen, (user_v, item_v), bend_v, label_v, slopes)

    def run_exactly(number):
        these = slice(0, number * per)
        get_user_w.wait()
        for slot in range(number):
            get_rows(0, slot).wait()
        run_user(these, user_rows, user_w, user_v, bend_v)
        get_item_w.wait()
        for slot in range(number):
            get_rows(1, slot).wait()
        run_item(these, item_rows, item_w, item_v)
        slopes_of(0, 0, number)
        add_terms(user_rows, user_slopes, targets, span, slice(0, head), these, 0, True)

    def run_groups():
        def of_group(work):
            def run(g, carry):
                work(g, pl.ds(pl.multiple_of(g * rows, rows), rows))
                return carry

            return lambda: lax.fori_loop(0, groups, run, 0)

        def await_rows(tower):
            def wait(slot, carry):
                get_rows(tower, slot).wait()
                return carry

            lax.fori_loop(0, live, wait, 0)

        get_user_w.wait()
        await_rows(0)
        of_group(lambda g, these: run_user(these, user_rows, user_w, user_v, bend_v))()
        get_item_w.wait()
        await_rows(1)
        of_group(lambda g, these: run_item(these, item_rows, item_w, item_v))()
        of_group(lambda g, these: slopes_of(pl.multiple_of(g * rows, rows), g * group, group))()
        sum_terms(user_rows, user_slopes, targets, span, slice(0, head), groups, rows, 0)

    exact = min(EXACT, clients)
    for number in range(1, exact + 1):
        pl.when(live == number)(functools.partial(run_exactly, number))
    if exact < clients:
        pl.when(live > exact)(run_groups)


def terms_kernel(sizes, user_rows, item_rows, user_slopes, item_slopes, count_v, after, give, *keeps):
    rows, shards, flip, skip = sizes
    del after
    groups = jnp.max(count_v[...]).astype(jnp.int32)
    span = user_rows.shape[1] // shards
    width = user_slopes.shape[1]
    towers = ((user_rows, user_slopes, slice(skip, width)), (item_rows, item_slopes, slice(0, width)))
    at = 0
    for tower, (feats, slopes, cols) in enumerate(towers):
        sum_terms(feats, slopes, ((relative_blocks(shards, flip ^ 1), give),), span, cols, groups, rows, at)
        sum_terms(feats, slopes, ((relative_blocks(shards, flip), keeps[tower]),), span, cols, groups, rows, 0)
        at += cols.stop - cols.start


def loss_kernel(sizes, ids_v, user_feats, item_feats, user_weight, item_weight, after, loss_v, user_v, item_v):
    per, group = sizes
    del after
    g = pl.program_id(0)
    mine = lax.axis_index("cluster")
    temper = 1.0 / math.sqrt(user_v.shape[1])
    everything = slice(0, group * per)
    run_user(everything, user_feats, user_weight.at[0], user_v, None)
    run_item(everything, item_feats, item_weight.at[0], item_v)
    lane = lax.broadcasted_iota(jnp.int32, loss_v.shape, 1)
    row = lax.broadcasted_iota(jnp.int32, loss_v.shape, 0)
    _, _, scores = scores_of((user_v, item_v), [i * per for i in range(group)], per, temper)
    losses = jnp.where(g == 0, 0.0, loss_v[...])
    for i, score in enumerate(scores):
        client = g * group + i
        labels = label_block(ids_v, client, per)
        soft = jnp.maximum(score, 0.0) + jnp.log1p(jnp.exp(-jnp.abs(score)))
        pair = soft - labels * score
        loss = jnp.sum(jnp.sum(pair, axis=1, keepdims=True), axis=0, keepdims=True) / (per * per)
        losses = jnp.where((row == mine) & (lane == client), loss, losses)
    loss_v[...] = losses


def swapped(value, axis, mask, size):
    return lax.ppermute(value, axis, [(i, i ^ mask) for i in range(size)])


def in_vmem(value):
    return pltpu.with_memory_space_constraint(value, pltpu.VMEM)


def in_hbm(*values):
    return [pltpu.with_memory_space_constraint(value, pltpu.HBM) for value in values]


def body(sizes, user_feats, item_feats, item_ids, picks, user_weight, item_weight):
    shards, clusters = sizes
    clients = picks.shape[0]
    row_count, depth = user_feats.shape
    per = row_count // clients
    width = user_weight.shape[2]
    group = math.gcd(clients, GROUP)
    rows = group * per
    head = width // 2
    top = shards // 2
    quarter = depth // 4
    table_rows = -(-clusters // 8) * 8
    assert shards & (shards - 1) == 0 and shards >= 4 and per <= LANES and clients <= LANES

    ids = item_ids.reshape(-1, LANES)
    bf16, f32, i32 = jnp.bfloat16, jnp.float32, jnp.int32
    hbm = pl.BlockSpec(memory_space=pltpu.HBM)
    anywhere = pl.BlockSpec(memory_space=pl.ANY)
    vmem = pl.BlockSpec(memory_space=pltpu.VMEM)
    flops = 2 * rows * depth * width

    def cost(factor):
        return pl.CostEstimate(flops=int(factor * flops), bytes_accessed=1 << 20, transcendentals=0)

    def params(mib):
        return pltpu.CompilerParams(vmem_limit_bytes=mib << 20)

    user_rows, item_rows, user_slopes, item_slopes, count, give, keep = pl.pallas_call(
        functools.partial(first_kernel, (clients, per, group, shards, head)),
        out_shape=[
            pltpu.VMEM((row_count, depth), bf16),
            pltpu.VMEM((row_count, depth), bf16),
            pltpu.VMEM((row_count, width), bf16),
            pltpu.VMEM((row_count, width), bf16),
            pltpu.VMEM((8, LANES), f32),
            pltpu.VMEM((quarter, head), f32),
            pltpu.VMEM((quarter, head), f32),
        ],
        in_specs=[hbm] * 6,
        out_specs=[vmem] * 7,
        scratch_shapes=[
            pltpu.SMEM((clients,), i32),
            pltpu.SMEM((clients + 1,), i32),
            pltpu.VMEM(ids.shape, i32),
            pltpu.VMEM((row_count, LANES), f32),
            pltpu.VMEM((depth, width), bf16),
            pltpu.VMEM((depth, width), bf16),
            pltpu.VMEM((row_count, width), f32),
            pltpu.VMEM((row_count, width), bf16),
            pltpu.VMEM((row_count, width), bf16),
            pltpu.SemaphoreType.DMA((2,)),
            pltpu.SemaphoreType.DMA((2,)),
            pltpu.SemaphoreType.DMA((2, clients)),
        ],
        compiler_params=params(24),
        cost_estimate=cost(6),
        name="first",
    )(*in_hbm(picks, ids, user_feats, item_feats, user_weight, item_weight))

    def terms(flip, skip, after):
        return pl.pallas_call(
            functools.partial(terms_kernel, (rows, shards, flip, skip)),
            out_shape=[
                pltpu.VMEM((quarter, 2 * width - skip), f32),
                pltpu.VMEM((quarter, width - skip), f32),
                pltpu.VMEM((quarter, width), f32),
            ],
            in_specs=[vmem] * 5 + [anywhere],
            out_specs=[vmem] * 3,
            compiler_params=params(8),
            cost_estimate=cost(2),
        )(in_vmem(user_rows), in_vmem(item_rows), in_vmem(user_slopes), in_vmem(item_slopes), in_vmem(count), after)

    def swap(value, axis, mask):
        return swapped(value, axis, mask, shards if axis == "client" else clusters)

    first_sum = swap(give, "client", 1) + keep
    from_first = swap(first_sum, "client", top)

    give, keep_user, keep_item = terms(top, head, count)
    got = swap(give, "client", 1)
    second_sum = got[:, : width - head] + keep_user
    third_sum = got[:, width - head :] + keep_item
    from_second = swap(second_sum, "client", top)
    from_third = swap(third_sum, "client", top)

    give, keep_user, keep_item = terms(0, 0, first_sum)
    got = swap(give, "client", 1)

    whole = lambda *shape: pl.BlockSpec(shape, lambda g: (0,) * len(shape))
    loss = pl.pallas_call(
        functools.partial(loss_kernel, (per, group)),
        grid=(clients // group,),
        out_shape=jax.ShapeDtypeStruct((table_rows, LANES), f32),
        in_specs=[
            whole(*ids.shape),
            pl.BlockSpec((rows, depth), lambda g: (g, 0)),
            pl.BlockSpec((rows, depth), lambda g: (g, 0)),
            whole(1, depth, width),
            whole(1, depth, width),
            anywhere,
        ],
        out_specs=whole(table_rows, LANES),
        scratch_shapes=[pltpu.VMEM((rows, width), bf16), pltpu.VMEM((rows, width), bf16)],
        compiler_params=params(24),
        cost_estimate=cost(8),
        name="loss",
    )(*in_hbm(ids, user_feats, item_feats, user_weight, item_weight), third_sum)
    home_user = got[:, :width] + keep_user
    home_item = got[:, width:] + keep_item
    loss, home_user, home_item = lax.optimization_barrier((loss, home_user, home_item))
    mask = 1
    while mask < clusters:
        loss = loss + swap(loss, "cluster", mask)
        mask *= 2
    loss_table = loss[:clusters, :clients].T

    user_grad = home_user + jnp.concatenate([from_first, from_second], axis=1)
    from_third, user_grad = lax.optimization_barrier((from_third, user_grad))
    item_grad = home_item + from_third
    half = shards // 4
    while half > 1:
        half //= 2
        cut = half * (depth // shards)
        mask = half << 1
        user_grad = user_grad[:cut] + swapped(user_grad[cut:], "client", mask, shards)
        item_grad = item_grad[:cut] + swapped(item_grad[cut:], "client", mask, shards)
    return loss_table, user_grad[None], item_grad[None]


def solution(mesh):
    in_specs = (
        P("client", None),
        P("client", None),
        P("client"),
        P("client"),
        P("cluster", None, None),
        P("cluster", None, None),
    )
    out_specs = (P("client", None), P("cluster", "client", None), P("cluster", "client", None))
    sizes = (mesh.shape["client"], mesh.shape["cluster"])
    return jax.shard_map(
        functools.partial(body, sizes), mesh=mesh, in_specs=in_specs, out_specs=out_specs, check_vma=False
    )
```

```python
import functools
import math

import jax
import jax.numpy as jnp
from jax import lax
from jax.experimental import pallas as pl
from jax.experimental.pallas import tpu as pltpu
from jax.sharding import PartitionSpec as P


GROUP = 4
EXACT = 8
HEAD = 4
LANES = 128


def contract_rows(left, right):
    return lax.dot_general(
        left, right, (((0,), (0,)), ((), ())), preferred_element_type=jnp.float32
    )


def contract_lanes(left, right):
    return lax.dot_general(
        left, right, (((1,), (1,)), ((), ())), preferred_element_type=jnp.float32
    )


def dot(left, right):
    return jnp.dot(left, right, preferred_element_type=jnp.float32)


def order_clients(picks_s, slots_s, clients, mine):
    chosen = jnp.int32(0)
    for c in range(clients):
        slots_s[chosen] = jnp.int32(c)
        chosen = chosen + (picks_s[c] == mine).astype(jnp.int32)
    last = chosen
    for c in range(clients):
        slots_s[last] = jnp.int32(c)
        last = last + (picks_s[c] != mine).astype(jnp.int32)
    return chosen


def label_block(ids_v, client, per):
    start = client * per
    row_at, off = start // LANES, start % LANES
    next_at = jnp.minimum(row_at + 1, ids_v.shape[0] - 1)
    lane = lax.broadcasted_iota(jnp.int32, (1, LANES), 1)
    turn = (LANES - off) % LANES
    here = pltpu.roll(ids_v[pl.ds(row_at, 1), :], turn, 1)
    there = pltpu.roll(ids_v[pl.ds(next_at, 1), :], turn, 1)
    row = jnp.where(lane < LANES - off, here, there).astype(jnp.float32)
    wide = jnp.broadcast_to(row, (per, LANES))
    diagonal = lax.broadcasted_iota(jnp.int32, (per, LANES), 0) == lax.broadcasted_iota(
        jnp.int32, (per, LANES), 1
    )
    column = jnp.sum(jnp.where(diagonal, wide, 0.0), axis=1, keepdims=True)
    return jnp.where(wide[:, :per] == column, 1.0, 0.0)


def run_user(at, feats, weight, user_v, bend_v):
    pre = dot(feats[at, :], weight[...])
    sig = jax.nn.sigmoid(pre)
    user_v[at, :] = (pre * sig).astype(jnp.bfloat16)
    if bend_v is not None:
        bend_v[at, :] = sig * (1.0 + pre * (1.0 - sig))


def run_item(at, feats, weight, item_v):
    item_v[at, :] = dot(feats[at, :], weight[...]).astype(jnp.bfloat16)


def scores_of(vectors, starts, per, temper):
    user_v, item_v = vectors
    users = [user_v[pl.ds(start, per), :] for start in starts]
    items = [item_v[pl.ds(start, per), :] for start in starts]
    scores = [contract_lanes(user, item) * temper for user, item in zip(users, items)]
    return users, items, scores


def run_item_slopes(base, slot, group, per, chosen, vectors, label_v, slope_v, item_slopes):
    temper = 1.0 / math.sqrt(item_slopes.shape[1])
    starts = [base + i * per for i in range(group)]
    users, _, scores = scores_of(vectors, starts, per, temper)
    slopes = [
        ((jax.nn.sigmoid(score) - label_v[pl.ds(start, per), :per]) * jnp.where(slot + i < chosen, temper, 0.0)).astype(
            jnp.bfloat16
        )
        for i, (score, start) in enumerate(zip(scores, starts))
    ]
    for slope, user, start in zip(slopes, users, starts):
        item_slopes[pl.ds(start, per), :] = contract_rows(slope, user).astype(jnp.bfloat16)
        slope_v[pl.ds(start, per), :per] = slope


def run_user_slopes(base, group, per, slope_v, item_v, bend_v, user_slopes):
    for i in range(group):
        at = pl.ds(base + i * per, per)
        user_slopes[at, :] = (dot(slope_v[at, :per], item_v[at, :]) * bend_v[at, :]).astype(jnp.bfloat16)


def add_terms(feats, slopes, targets, span, cols, these, at, fresh):
    wide = cols.stop - cols.start
    for blocks, out in targets:
        for j, block in enumerate(blocks):
            place = (slice(j * span, (j + 1) * span), slice(at, at + wide))
            part_of = pl.ds(pl.multiple_of(block * span, span), span)
            part = contract_rows(feats[these, part_of], slopes[these, cols])
            out[place] = part if fresh else out[place] + part


def sum_terms(feats, slopes, targets, span, cols, groups, rows, at):
    @pl.when(groups == 1)
    def _():
        add_terms(feats, slopes, targets, span, cols, slice(0, rows), at, True)

    @pl.when(groups > 1)
    def _():
        add_terms(feats, slopes, targets, span, cols, slice(0, 2 * rows), at, True)

        def more(g, carry):
            add_terms(feats, slopes, targets, span, cols, pl.ds(pl.multiple_of(g * rows, rows), rows), at, False)
            return carry

        lax.fori_loop(2, groups, more, 0)


def relative_blocks(shards, flip):
    me = lax.axis_index("client")
    return [jnp.bitwise_xor(me, (j << 1) ^ flip) for j in range(shards // 4)]


def first_kernel(
    sizes, picks, ids_h, user_feats, item_feats, user_weight, item_weight,
    user_rows, item_rows, slope_v, bend_v, item_v, item_slopes, count_v, give, keep,
    picks_s, slots_s, ids_v, label_v, user_w, item_w, user_v, small_sem, weight_sem, feat_sem,
):
    clients, per, group, shards, head = sizes
    rows = group * per
    mine = lax.axis_index("cluster")
    get_picks = pltpu.make_async_copy(picks, picks_s, small_sem.at[0])
    get_ids = pltpu.make_async_copy(ids_h, ids_v, small_sem.at[1])
    get_user_w = pltpu.make_async_copy(user_weight.at[0], user_w, weight_sem.at[0])
    get_item_w = pltpu.make_async_copy(item_weight.at[0], item_w, weight_sem.at[1])
    get_picks.start()
    get_user_w.start()
    get_ids.start()
    get_picks.wait()
    chosen = order_clients(picks_s, slots_s, clients, mine)
    live = jnp.maximum(1, chosen)
    groups = (live + group - 1) // group
    feats = (user_rows, item_rows)

    def place_of(slot):
        return pl.ds(pl.multiple_of(slot * per, per), per)

    def get_rows(tower, slot):
        source = (user_feats, item_feats)[tower]
        return pltpu.make_async_copy(
            source.at[place_of(slots_s[slot]), :], feats[tower].at[place_of(slot), :], feat_sem.at[tower, slot]
        )

    def start_rows(tower):
        def start(slot, carry):
            get_rows(tower, slot).start()
            return carry

        lax.fori_loop(0, live, start, 0)

    start_rows(0)
    count_v[...] = jnp.broadcast_to(groups.astype(jnp.float32), count_v.shape)

    def clear(slot, carry):
        for ref in (user_rows, item_rows, slope_v, bend_v, item_v, item_slopes):
            ref[place_of(slot), :] = jnp.zeros((per, ref.shape[1]), ref.dtype)
        return carry

    lax.fori_loop(live, groups * group, clear, 0)
    get_ids.wait()

    def label_group(g, carry):
        for i in range(group):
            slot = g * group + i
            label_v[place_of(slot), :per] = label_block(ids_v, slots_s[slot], per)
        return carry

    lax.fori_loop(0, groups, label_group, 0)
    get_user_w.wait()
    get_item_w.start()

    top = shards // 2
    span = user_rows.shape[1] // shards
    targets = ((relative_blocks(shards, top ^ 1), give), (relative_blocks(shards, top), keep))

    def slopes_of(base, slot, number):
        run_item_slopes(base, slot, number, per, chosen, (user_v, item_v), label_v, slope_v, item_slopes)

    def run_exactly(number):
        these = slice(0, number * per)
        for slot in range(number):
            get_rows(0, slot).wait()
        start_rows(1)
        run_user(these, user_rows, user_w, user_v, bend_v)
        get_item_w.wait()
        for slot in range(number):
            get_rows(1, slot).wait()
        run_item(these, item_rows, item_w, item_v)
        slopes_of(0, 0, number)
        add_terms(item_rows, item_slopes, targets, span, slice(0, head), these, 0, True)

    def run_groups():
        def of_group(work):
            def run(g, carry):
                work(g, pl.ds(pl.multiple_of(g * rows, rows), rows))
                return carry

            return lambda: lax.fori_loop(0, groups, run, 0)

        def await_rows(tower):
            def wait(slot, carry):
                get_rows(tower, slot).wait()
                return carry

            lax.fori_loop(0, live, wait, 0)

        await_rows(0)
        start_rows(1)
        of_group(lambda g, these: run_user(these, user_rows, user_w, user_v, bend_v))()
        get_item_w.wait()
        await_rows(1)
        of_group(lambda g, these: run_item(these, item_rows, item_w, item_v))()
        of_group(lambda g, these: slopes_of(pl.multiple_of(g * rows, rows), g * group, group))()
        sum_terms(item_rows, item_slopes, targets, span, slice(0, head), groups, rows, 0)

    exact = min(EXACT, clients)
    for number in range(1, exact + 1):
        pl.when(live == number)(functools.partial(run_exactly, number))
    if exact < clients:
        pl.when(live > exact)(run_groups)


def both_targets(shards, flip, give, keep):
    return ((relative_blocks(shards, flip ^ 1), give), (relative_blocks(shards, flip), keep))


def groups_of(count_v):
    return jnp.max(count_v[...]).astype(jnp.int32)


def item_kernel(sizes, item_rows, item_slopes, count_v, after, give, keep):
    rows, shards, head = sizes
    del after
    cols = slice(head, item_slopes.shape[1])
    targets = both_targets(shards, shards // 2, give, keep)
    sum_terms(item_rows, item_slopes, targets, item_rows.shape[1] // shards, cols, groups_of(count_v), rows, 0)


def user_kernel(sizes, user_rows, slope_v, bend_v, item_v, count_v, user_slopes, give, keep):
    per, rows, shards = sizes
    groups = groups_of(count_v)

    def slopes(g, carry):
        run_user_slopes(pl.multiple_of(g * rows, rows), rows // per, per, slope_v, item_v, bend_v, user_slopes)
        return carry

    lax.fori_loop(0, groups, slopes, 0)
    targets = both_targets(shards, shards // 2, give, keep)
    cols = slice(0, user_slopes.shape[1])
    sum_terms(user_rows, user_slopes, targets, user_rows.shape[1] // shards, cols, groups, rows, 0)


def home_kernel(sizes, user_rows, item_rows, user_slopes, item_slopes, count_v, after, give, keep_user, keep_item):
    rows, shards = sizes
    del after
    groups = groups_of(count_v)
    width = user_slopes.shape[1]
    towers = ((user_rows, user_slopes, keep_user), (item_rows, item_slopes, keep_item))
    for tower, (feats, slopes, keep) in enumerate(towers):
        span = feats.shape[1] // shards
        cols = slice(0, width)
        sum_terms(feats, slopes, ((relative_blocks(shards, 1), give),), span, cols, groups, rows, tower * width)
        sum_terms(feats, slopes, ((relative_blocks(shards, 0), keep),), span, cols, groups, rows, 0)


def loss_kernel(sizes, ids_v, user_feats, item_feats, user_weight, item_weight, after, loss_v, user_v, item_v):
    per, group = sizes
    del after
    g = pl.program_id(0)
    mine = lax.axis_index("cluster")
    temper = 1.0 / math.sqrt(user_v.shape[1])
    everything = slice(0, group * per)
    run_user(everything, user_feats, user_weight.at[0], user_v, None)
    run_item(everything, item_feats, item_weight.at[0], item_v)
    lane = lax.broadcasted_iota(jnp.int32, loss_v.shape, 1)
    row = lax.broadcasted_iota(jnp.int32, loss_v.shape, 0)
    _, _, scores = scores_of((user_v, item_v), [i * per for i in range(group)], per, temper)
    losses = jnp.where(g == 0, 0.0, loss_v[...])
    for i, score in enumerate(scores):
        client = g * group + i
        labels = label_block(ids_v, client, per)
        soft = jnp.maximum(score, 0.0) + jnp.log1p(jnp.exp(-jnp.abs(score)))
        pair = soft - labels * score
        loss = jnp.sum(jnp.sum(pair, axis=1, keepdims=True), axis=0, keepdims=True) / (per * per)
        losses = jnp.where((row == mine) & (lane == client), loss, losses)
    loss_v[...] = losses


def swapped(value, axis, mask, size):
    return lax.ppermute(value, axis, [(i, i ^ mask) for i in range(size)])


def in_vmem(value):
    return pltpu.with_memory_space_constraint(value, pltpu.VMEM)


def in_hbm(*values):
    return [pltpu.with_memory_space_constraint(value, pltpu.HBM) for value in values]


def body(sizes, user_feats, item_feats, item_ids, picks, user_weight, item_weight):
    shards, clusters = sizes
    clients = picks.shape[0]
    row_count, depth = user_feats.shape
    per = row_count // clients
    width = user_weight.shape[2]
    group = math.gcd(clients, GROUP)
    rows = group * per
    head = width // HEAD
    top = shards // 2
    quarter = depth // 4
    table_rows = -(-clusters // 8) * 8
    assert shards & (shards - 1) == 0 and shards >= 4 and per <= LANES and clients <= LANES

    ids = item_ids.reshape(-1, LANES)
    bf16, f32, i32 = jnp.bfloat16, jnp.float32, jnp.int32
    hbm = pl.BlockSpec(memory_space=pltpu.HBM)
    anywhere = pl.BlockSpec(memory_space=pl.ANY)
    vmem = pl.BlockSpec(memory_space=pltpu.VMEM)
    flops = 2 * rows * depth * width

    def cost(factor):
        return pl.CostEstimate(flops=int(factor * flops), bytes_accessed=1 << 20, transcendentals=0)

    def params(mib):
        return pltpu.CompilerParams(vmem_limit_bytes=mib << 20)

    def kernel(function, outs, ins, mib, factor, **more):
        return pl.pallas_call(
            function,
            out_shape=[pltpu.VMEM(shape, dtype) for shape, dtype in outs],
            out_specs=[vmem] * len(outs),
            compiler_params=params(mib),
            cost_estimate=cost(factor),
            **more,
        )(*ins)

    user_rows, item_rows, slope, bend, item_vec, item_slopes, count, give, keep = kernel(
        functools.partial(first_kernel, (clients, per, group, shards, head)),
        [
            ((row_count, depth), bf16),
            ((row_count, depth), bf16),
            ((row_count, LANES), bf16),
            ((row_count, width), f32),
            ((row_count, width), bf16),
            ((row_count, width), bf16),
            ((8, LANES), f32),
            ((quarter, head), f32),
            ((quarter, head), f32),
        ],
        in_hbm(picks, ids, user_feats, item_feats, user_weight, item_weight),
        16,
        6,
        in_specs=[hbm] * 6,
        scratch_shapes=[
            pltpu.SMEM((clients,), i32),
            pltpu.SMEM((clients + 1,), i32),
            pltpu.VMEM(ids.shape, i32),
            pltpu.VMEM((row_count, LANES), f32),
            pltpu.VMEM((depth, width), bf16),
            pltpu.VMEM((depth, width), bf16),
            pltpu.VMEM((row_count, width), bf16),
            pltpu.SemaphoreType.DMA((2,)),
            pltpu.SemaphoreType.DMA((2,)),
            pltpu.SemaphoreType.DMA((2, clients)),
        ],
    )
    user_rows, item_rows, slope, bend, item_vec, item_slopes, count = map(
        in_vmem, (user_rows, item_rows, slope, bend, item_vec, item_slopes, count)
    )

    def swap(value, axis, mask):
        return swapped(value, axis, mask, shards if axis == "client" else clusters)

    first_sum = swap(give, "client", 1) + keep
    from_first = swap(first_sum, "client", top)

    rest = (quarter, width - head)
    give, keep = kernel(
        functools.partial(item_kernel, (rows, shards, head)),
        [(rest, f32), (rest, f32)],
        (item_rows, item_slopes, count, first_sum),
        6,
        1,
        in_specs=[vmem] * 3 + [anywhere],
    )
    second_sum = swap(give, "client", 1) + keep
    from_second = swap(second_sum, "client", top)

    user_slopes, give, keep = kernel(
        functools.partial(user_kernel, (per, rows, shards)),
        [((row_count, width), bf16), ((quarter, width), f32), ((quarter, width), f32)],
        (user_rows, slope, bend, item_vec, count),
        6,
        1,
        in_specs=[vmem] * 5,
    )
    user_slopes = in_vmem(user_slopes)
    third_sum = swap(give, "client", 1) + keep
    from_third = swap(third_sum, "client", top)

    give, keep_user, keep_item = kernel(
        functools.partial(home_kernel, (rows, shards)),
        [((quarter, 2 * width), f32), ((quarter, width), f32), ((quarter, width), f32)],
        (user_rows, item_rows, user_slopes, item_slopes, count, second_sum),
        8,
        2,
        in_specs=[vmem] * 5 + [anywhere],
    )
    got = swap(give, "client", 1)

    whole = lambda *shape: pl.BlockSpec(shape, lambda g: (0,) * len(shape))
    loss = pl.pallas_call(
        functools.partial(loss_kernel, (per, group)),
        grid=(clients // group,),
        out_shape=jax.ShapeDtypeStruct((table_rows, LANES), f32),
        in_specs=[
            whole(*ids.shape),
            pl.BlockSpec((rows, depth), lambda g: (g, 0)),
            pl.BlockSpec((rows, depth), lambda g: (g, 0)),
            whole(1, depth, width),
            whole(1, depth, width),
            anywhere,
        ],
        out_specs=whole(table_rows, LANES),
        scratch_shapes=[pltpu.VMEM((rows, width), bf16), pltpu.VMEM((rows, width), bf16)],
        compiler_params=params(24),
        cost_estimate=cost(8),
        name="loss",
    )(*in_hbm(ids, user_feats, item_feats, user_weight, item_weight), third_sum)
    home_user = got[:, :width] + keep_user
    home_item = got[:, width:] + keep_item
    loss, home_user, home_item = lax.optimization_barrier((loss, home_user, home_item))
    mask = 1
    while mask < clusters:
        loss = loss + swap(loss, "cluster", mask)
        mask *= 2
    loss_table = loss[:clusters, :clients].T

    item_grad = home_item + jnp.concatenate([from_first, from_second], axis=1)
    from_third, item_grad = lax.optimization_barrier((from_third, item_grad))
    user_grad = home_user + from_third
    half = shards // 4
    while half > 1:
        half //= 2
        cut = half * (depth // shards)
        mask = half << 1
        user_grad = user_grad[:cut] + swapped(user_grad[cut:], "client", mask, shards)
        item_grad = item_grad[:cut] + swapped(item_grad[cut:], "client", mask, shards)
    return loss_table, user_grad[None], item_grad[None]


def solution(mesh):
    in_specs = (
        P("client", None),
        P("client", None),
        P("client"),
        P("client"),
        P("cluster", None, None),
        P("cluster", None, None),
    )
    out_specs = (P("client", None), P("cluster", "client", None), P("cluster", "client", None))
    sizes = (mesh.shape["client"], mesh.shape["cluster"])
    return jax.shard_map(
        functools.partial(body, sizes), mesh=mesh, in_specs=in_specs, out_specs=out_specs, check_vma=False
    )
```

```python
import functools
import math

import jax
import jax.numpy as jnp
from jax import lax
from jax.experimental import pallas as pl
from jax.experimental.pallas import tpu as pltpu
from jax.sharding import PartitionSpec as P


GROUP = 4
EXACT = 8
HEAD = 4
LANES = 128


def contract_rows(left, right):
    return lax.dot_general(
        left, right, (((0,), (0,)), ((), ())), preferred_element_type=jnp.float32
    )


def contract_lanes(left, right):
    return lax.dot_general(
        left, right, (((1,), (1,)), ((), ())), preferred_element_type=jnp.float32
    )


def dot(left, right):
    return jnp.dot(left, right, preferred_element_type=jnp.float32)


def order_clients(picks_s, slots_s, clients, mine):
    chosen = jnp.int32(0)
    for c in range(clients):
        slots_s[chosen] = jnp.int32(c)
        chosen = chosen + (picks_s[c] == mine).astype(jnp.int32)
    last = chosen
    for c in range(clients):
        slots_s[last] = jnp.int32(c)
        last = last + (picks_s[c] != mine).astype(jnp.int32)
    return chosen


def label_block(ids_v, client, per):
    start = client * per
    row_at, off = start // LANES, start % LANES
    next_at = jnp.minimum(row_at + 1, ids_v.shape[0] - 1)
    lane = lax.broadcasted_iota(jnp.int32, (1, LANES), 1)
    turn = (LANES - off) % LANES
    here = pltpu.roll(ids_v[pl.ds(row_at, 1), :], turn, 1)
    there = pltpu.roll(ids_v[pl.ds(next_at, 1), :], turn, 1)
    row = jnp.where(lane < LANES - off, here, there).astype(jnp.float32)
    wide = jnp.broadcast_to(row, (per, LANES))
    diagonal = lax.broadcasted_iota(jnp.int32, (per, LANES), 0) == lax.broadcasted_iota(
        jnp.int32, (per, LANES), 1
    )
    column = jnp.sum(jnp.where(diagonal, wide, 0.0), axis=1, keepdims=True)
    return jnp.where(wide[:, :per] == column, 1.0, 0.0)


def run_user(at, feats, weight, user_v, bend_v):
    pre = dot(feats[at, :], weight[...])
    sig = jax.nn.sigmoid(pre)
    user_v[at, :] = (pre * sig).astype(jnp.bfloat16)
    if bend_v is not None:
        bend_v[at, :] = sig * (1.0 + pre * (1.0 - sig))


def run_item(at, feats, weight, item_v):
    item_v[at, :] = dot(feats[at, :], weight[...]).astype(jnp.bfloat16)


def scores_of(vectors, starts, per, temper):
    user_v, item_v = vectors
    users = [user_v[pl.ds(start, per), :] for start in starts]
    items = [item_v[pl.ds(start, per), :] for start in starts]
    scores = [contract_lanes(user, item) * temper for user, item in zip(users, items)]
    return users, items, scores


def run_item_slopes(base, slot, group, per, chosen, vectors, label_v, slope_v, item_slopes):
    temper = 1.0 / math.sqrt(item_slopes.shape[1])
    starts = [base + i * per for i in range(group)]
    users, _, scores = scores_of(vectors, starts, per, temper)
    slopes = [
        ((jax.nn.sigmoid(score) - label_v[pl.ds(start, per), :per]) * jnp.where(slot + i < chosen, temper, 0.0)).astype(
            jnp.bfloat16
        )
        for i, (score, start) in enumerate(zip(scores, starts))
    ]
    for slope, user, start in zip(slopes, users, starts):
        item_slopes[pl.ds(start, per), :] = contract_rows(slope, user).astype(jnp.bfloat16)
        slope_v[pl.ds(start, per), :per] = slope


def run_user_slopes(base, group, per, slope_v, item_v, bend_v, user_slopes):
    for i in range(group):
        at = pl.ds(base + i * per, per)
        user_slopes[at, :] = (dot(slope_v[at, :per], item_v[at, :]) * bend_v[at, :]).astype(jnp.bfloat16)


def add_terms(feats, slopes, targets, span, cols, these, at, fresh):
    wide = cols.stop - cols.start
    for blocks, out in targets:
        for j, block in enumerate(blocks):
            place = (slice(j * span, (j + 1) * span), slice(at, at + wide))
            part_of = pl.ds(pl.multiple_of(block * span, span), span)
            part = contract_rows(feats[these, part_of], slopes[these, cols])
            out[place] = part if fresh else out[place] + part


def sum_terms(feats, slopes, targets, span, cols, groups, rows, at):
    @pl.when(groups == 1)
    def _():
        add_terms(feats, slopes, targets, span, cols, slice(0, rows), at, True)

    @pl.when(groups > 1)
    def _():
        add_terms(feats, slopes, targets, span, cols, slice(0, 2 * rows), at, True)

        def more(g, carry):
            add_terms(feats, slopes, targets, span, cols, pl.ds(pl.multiple_of(g * rows, rows), rows), at, False)
            return carry

        lax.fori_loop(2, groups, more, 0)


def relative_blocks(shards, flip):
    me = lax.axis_index("client")
    return [jnp.bitwise_xor(me, (j << 1) ^ flip) for j in range(shards // 4)]


def first_kernel(
    sizes, picks, ids_h, user_feats, item_feats, user_weight, item_weight,
    user_rows, item_rows, slope_v, bend_v, item_v, item_slopes, count_v, give, keep,
    picks_s, slots_s, ids_v, label_v, user_w, item_w, user_v, small_sem, weight_sem, feat_sem,
):
    clients, per, group, shards, head = sizes
    rows = group * per
    mine = lax.axis_index("cluster")
    get_picks = pltpu.make_async_copy(picks, picks_s, small_sem.at[0])
    get_ids = pltpu.make_async_copy(ids_h, ids_v, small_sem.at[1])
    get_user_w = pltpu.make_async_copy(user_weight.at[0], user_w, weight_sem.at[0])
    get_item_w = pltpu.make_async_copy(item_weight.at[0], item_w, weight_sem.at[1])
    get_picks.start()
    get_user_w.start()
    get_ids.start()
    get_picks.wait()
    chosen = order_clients(picks_s, slots_s, clients, mine)
    live = jnp.maximum(1, chosen)
    groups = (live + group - 1) // group
    feats = (user_rows, item_rows)

    def place_of(slot):
        return pl.ds(pl.multiple_of(slot * per, per), per)

    def get_rows(tower, slot):
        source = (user_feats, item_feats)[tower]
        return pltpu.make_async_copy(
            source.at[place_of(slots_s[slot]), :], feats[tower].at[place_of(slot), :], feat_sem.at[tower, slot]
        )

    def start_rows(tower):
        def start(slot, carry):
            get_rows(tower, slot).start()
            return carry

        lax.fori_loop(0, live, start, 0)

    start_rows(0)
    count_v[...] = jnp.broadcast_to(groups.astype(jnp.float32), count_v.shape)

    def clear(slot, carry):
        for ref in (user_rows, item_rows, slope_v, bend_v, item_v, item_slopes):
            ref[place_of(slot), :] = jnp.zeros((per, ref.shape[1]), ref.dtype)
        return carry

    lax.fori_loop(live, groups * group, clear, 0)
    get_ids.wait()

    def label_group(g, carry):
        for i in range(group):
            slot = g * group + i
            label_v[place_of(slot), :per] = label_block(ids_v, slots_s[slot], per)
        return carry

    lax.fori_loop(0, groups, label_group, 0)
    get_user_w.wait()
    get_item_w.start()

    top = shards // 2
    span = user_rows.shape[1] // shards
    targets = ((relative_blocks(shards, top ^ 1), give), (relative_blocks(shards, top), keep))

    def slopes_of(base, slot, number):
        run_item_slopes(base, slot, number, per, chosen, (user_v, item_v), label_v, slope_v, item_slopes)

    def run_exactly(number):
        these = slice(0, number * per)
        for slot in range(number):
            get_rows(0, slot).wait()
        start_rows(1)
        run_user(these, user_rows, user_w, user_v, bend_v)
        get_item_w.wait()
        for slot in range(number):
            get_rows(1, slot).wait()
        run_item(these, item_rows, item_w, item_v)
        slopes_of(0, 0, number)
        add_terms(item_rows, item_slopes, targets, span, slice(0, head), these, 0, True)

    def run_groups():
        def of_group(work):
            def run(g, carry):
                work(g, pl.ds(pl.multiple_of(g * rows, rows), rows))
                return carry

            return lambda: lax.fori_loop(0, groups, run, 0)

        def await_rows(tower):
            def wait(slot, carry):
                get_rows(tower, slot).wait()
                return carry

            lax.fori_loop(0, live, wait, 0)

        await_rows(0)
        start_rows(1)
        of_group(lambda g, these: run_user(these, user_rows, user_w, user_v, bend_v))()
        get_item_w.wait()
        await_rows(1)
        of_group(lambda g, these: run_item(these, item_rows, item_w, item_v))()
        of_group(lambda g, these: slopes_of(pl.multiple_of(g * rows, rows), g * group, group))()
        sum_terms(item_rows, item_slopes, targets, span, slice(0, head), groups, rows, 0)

    exact = min(EXACT, clients)
    for number in range(1, exact + 1):
        pl.when(live == number)(functools.partial(run_exactly, number))
    if exact < clients:
        pl.when(live > exact)(run_groups)


def both_targets(shards, flip, give, keep):
    return ((relative_blocks(shards, flip ^ 1), give), (relative_blocks(shards, flip), keep))


def groups_of(count_v):
    return jnp.max(count_v[...]).astype(jnp.int32)


def item_kernel(sizes, item_rows, item_slopes, count_v, after, give, keep):
    rows, shards, head = sizes
    del after
    cols = slice(head, item_slopes.shape[1])
    targets = both_targets(shards, shards // 2, give, keep)
    sum_terms(item_rows, item_slopes, targets, item_rows.shape[1] // shards, cols, groups_of(count_v), rows, 0)


def user_kernel(sizes, user_rows, slope_v, bend_v, item_v, count_v, user_slopes, give, keep):
    per, rows, shards = sizes
    groups = groups_of(count_v)

    def slopes(g, carry):
        run_user_slopes(pl.multiple_of(g * rows, rows), rows // per, per, slope_v, item_v, bend_v, user_slopes)
        return carry

    lax.fori_loop(0, groups, slopes, 0)
    targets = both_targets(shards, shards // 2, give, keep)
    cols = slice(0, user_slopes.shape[1])
    sum_terms(user_rows, user_slopes, targets, user_rows.shape[1] // shards, cols, groups, rows, 0)


def home_kernel(sizes, user_rows, item_rows, user_slopes, item_slopes, count_v, after, give, keep_user, keep_item):
    rows, shards = sizes
    del after
    groups = groups_of(count_v)
    width = user_slopes.shape[1]
    towers = ((user_rows, user_slopes, keep_user), (item_rows, item_slopes, keep_item))
    for tower, (feats, slopes, keep) in enumerate(towers):
        span = feats.shape[1] // shards
        cols = slice(0, width)
        sum_terms(feats, slopes, ((relative_blocks(shards, 1), give),), span, cols, groups, rows, tower * width)
        sum_terms(feats, slopes, ((relative_blocks(shards, 0), keep),), span, cols, groups, rows, 0)


def loss_kernel(sizes, ids_v, user_feats, item_feats, user_weight, item_weight, after, loss_v, user_v, item_v):
    per, group = sizes
    del after
    g = pl.program_id(0)
    mine = lax.axis_index("cluster")
    temper = 1.0 / math.sqrt(user_v.shape[1])
    everything = slice(0, group * per)
    run_user(everything, user_feats, user_weight.at[0], user_v, None)
    run_item(everything, item_feats, item_weight.at[0], item_v)
    lane = lax.broadcasted_iota(jnp.int32, loss_v.shape, 1)
    row = lax.broadcasted_iota(jnp.int32, loss_v.shape, 0)
    _, _, scores = scores_of((user_v, item_v), [i * per for i in range(group)], per, temper)
    losses = jnp.where(g == 0, 0.0, loss_v[...])
    for i, score in enumerate(scores):
        client = g * group + i
        labels = label_block(ids_v, client, per)
        soft = jnp.maximum(score, 0.0) + jnp.log1p(jnp.exp(-jnp.abs(score)))
        pair = soft - labels * score
        loss = jnp.sum(jnp.sum(pair, axis=1, keepdims=True), axis=0, keepdims=True) / (per * per)
        losses = jnp.where((row == mine) & (lane == client), loss, losses)
    loss_v[...] = losses


def finish_kernel(start, home, piece, *refs):
    out, total, sem = refs[-3:]
    cols = slice(start, start + piece.shape[1])
    total[...] = home[:, cols] + piece[...]
    copy = pltpu.make_async_copy(total, out.at[:, cols], sem.at[0])
    copy.start()
    copy.wait()


def swapped(value, axis, mask, size):
    return lax.ppermute(value, axis, [(i, i ^ mask) for i in range(size)])


def in_vmem(value):
    return pltpu.with_memory_space_constraint(value, pltpu.VMEM)


def in_hbm(*values):
    return [pltpu.with_memory_space_constraint(value, pltpu.HBM) for value in values]


def body(sizes, user_feats, item_feats, item_ids, picks, user_weight, item_weight):
    shards, clusters = sizes
    clients = picks.shape[0]
    row_count, depth = user_feats.shape
    per = row_count // clients
    width = user_weight.shape[2]
    group = math.gcd(clients, GROUP)
    rows = group * per
    head = width // HEAD
    top = shards // 2
    quarter = depth // 4
    table_rows = -(-clusters // 8) * 8
    assert shards & (shards - 1) == 0 and shards >= 4 and per <= LANES and clients <= LANES

    ids = item_ids.reshape(-1, LANES)
    bf16, f32, i32 = jnp.bfloat16, jnp.float32, jnp.int32
    hbm = pl.BlockSpec(memory_space=pltpu.HBM)
    anywhere = pl.BlockSpec(memory_space=pl.ANY)
    vmem = pl.BlockSpec(memory_space=pltpu.VMEM)
    flops = 2 * rows * depth * width

    def cost(factor):
        return pl.CostEstimate(flops=int(factor * flops), bytes_accessed=1 << 20, transcendentals=0)

    def params(mib):
        return pltpu.CompilerParams(vmem_limit_bytes=mib << 20)

    def kernel(function, outs, ins, mib, factor, **more):
        return pl.pallas_call(
            function,
            out_shape=[pltpu.VMEM(shape, dtype) for shape, dtype in outs],
            out_specs=[vmem] * len(outs),
            compiler_params=params(mib),
            cost_estimate=cost(factor),
            **more,
        )(*ins)

    user_rows, item_rows, slope, bend, item_vec, item_slopes, count, give, keep = kernel(
        functools.partial(first_kernel, (clients, per, group, shards, head)),
        [
            ((row_count, depth), bf16),
            ((row_count, depth), bf16),
            ((row_count, LANES), bf16),
            ((row_count, width), f32),
            ((row_count, width), bf16),
            ((row_count, width), bf16),
            ((8, LANES), f32),
            ((quarter, head), f32),
            ((quarter, head), f32),
        ],
        in_hbm(picks, ids, user_feats, item_feats, user_weight, item_weight),
        16,
        6,
        in_specs=[hbm] * 6,
        scratch_shapes=[
            pltpu.SMEM((clients,), i32),
            pltpu.SMEM((clients + 1,), i32),
            pltpu.VMEM(ids.shape, i32),
            pltpu.VMEM((row_count, LANES), f32),
            pltpu.VMEM((depth, width), bf16),
            pltpu.VMEM((depth, width), bf16),
            pltpu.VMEM((row_count, width), bf16),
            pltpu.SemaphoreType.DMA((2,)),
            pltpu.SemaphoreType.DMA((2,)),
            pltpu.SemaphoreType.DMA((2, clients)),
        ],
    )
    user_rows, item_rows, slope, bend, item_vec, item_slopes, count = map(
        in_vmem, (user_rows, item_rows, slope, bend, item_vec, item_slopes, count)
    )

    def swap(value, axis, mask):
        return swapped(value, axis, mask, shards if axis == "client" else clusters)

    first_sum = swap(give, "client", 1) + keep
    from_first = swap(first_sum, "client", top)

    rest = (quarter, width - head)
    give, keep = kernel(
        functools.partial(item_kernel, (rows, shards, head)),
        [(rest, f32), (rest, f32)],
        (item_rows, item_slopes, count, first_sum),
        6,
        1,
        in_specs=[vmem] * 3 + [anywhere],
    )
    second_sum = swap(give, "client", 1) + keep
    from_second = swap(second_sum, "client", top)

    user_slopes, give, keep = kernel(
        functools.partial(user_kernel, (per, rows, shards)),
        [((row_count, width), bf16), ((quarter, width), f32), ((quarter, width), f32)],
        (user_rows, slope, bend, item_vec, count),
        6,
        1,
        in_specs=[vmem] * 5,
    )
    user_slopes = in_vmem(user_slopes)
    third_sum = swap(give, "client", 1) + keep
    from_third = swap(third_sum[:, head:], "client", top)
    from_fourth = swap(third_sum[:, :head], "client", top)

    give, keep_user, keep_item = kernel(
        functools.partial(home_kernel, (rows, shards)),
        [((quarter, 2 * width), f32), ((quarter, width), f32), ((quarter, width), f32)],
        (user_rows, item_rows, user_slopes, item_slopes, count, second_sum),
        8,
        2,
        in_specs=[vmem] * 5 + [anywhere],
    )
    got = swap(give, "client", 1)

    whole = lambda *shape: pl.BlockSpec(shape, lambda g: (0,) * len(shape))
    loss = pl.pallas_call(
        functools.partial(loss_kernel, (per, group)),
        grid=(clients // group,),
        out_shape=jax.ShapeDtypeStruct((table_rows, LANES), f32),
        in_specs=[
            whole(*ids.shape),
            pl.BlockSpec((rows, depth), lambda g: (g, 0)),
            pl.BlockSpec((rows, depth), lambda g: (g, 0)),
            whole(1, depth, width),
            whole(1, depth, width),
            anywhere,
        ],
        out_specs=whole(table_rows, LANES),
        scratch_shapes=[pltpu.VMEM((rows, width), bf16), pltpu.VMEM((rows, width), bf16)],
        compiler_params=params(24),
        cost_estimate=cost(8),
        name="loss",
    )(*in_hbm(ids, user_feats, item_feats, user_weight, item_weight), third_sum)
    home_user = got[:, :width] + keep_user
    home_item = got[:, width:] + keep_item
    loss, home_user, home_item = lax.optimization_barrier((loss, home_user, home_item))
    mask = 1
    while mask < clusters:
        loss = loss + swap(loss, "cluster", mask)
        mask *= 2
    loss_table = loss[:clusters, :clients].T

    item_grad = home_item + jnp.concatenate([from_first, from_second], axis=1)
    from_third, item_grad = lax.optimization_barrier((from_third, item_grad))

    def finish(piece, start, *so_far):
        return pl.pallas_call(
            functools.partial(finish_kernel, start),
            out_shape=pltpu.HBM(home_user.shape, f32),
            in_specs=[vmem, vmem] + [hbm] * len(so_far),
            out_specs=hbm,
            scratch_shapes=[pltpu.VMEM(piece.shape, f32), pltpu.SemaphoreType.DMA((1,))],
            input_output_aliases={2: 0} if so_far else {},
            compiler_params=params(4),
            name="finish",
        )(in_vmem(home_user), in_vmem(piece), *so_far)

    most = finish(from_third, head)
    most, from_fourth = lax.optimization_barrier((most, from_fourth))
    user_grad = finish(from_fourth, 0, *in_hbm(most))
    half = shards // 4
    while half > 1:
        half //= 2
        cut = half * (depth // shards)
        mask = half << 1
        user_grad = user_grad[:cut] + swapped(user_grad[cut:], "client", mask, shards)
        item_grad = item_grad[:cut] + swapped(item_grad[cut:], "client", mask, shards)
    return loss_table, user_grad[None], item_grad[None]


def solution(mesh):
    in_specs = (
        P("client", None),
        P("client", None),
        P("client"),
        P("client"),
        P("cluster", None, None),
        P("cluster", None, None),
    )
    out_specs = (P("client", None), P("cluster", "client", None), P("cluster", "client", None))
    sizes = (mesh.shape["client"], mesh.shape["cluster"])
    return jax.shard_map(
        functools.partial(body, sizes), mesh=mesh, in_specs=in_specs, out_specs=out_specs, check_vma=False
    )
```
